32 devices in a mesh: row: 4 (over y, core), col: 8 (over z, x).
Axes of the slice: x: 2, y: 2, z: 4, core: 2. Of those that a mesh axis runs over, the one named last changes fastest.
Arguments:
- right_side: float32 [32768], P(('row', 'col')), may hold values from -6 to 6
- eigen_basis: bfloat16 [12288, 512], P(('row', 'col')), may hold values from -0.0546875 to 0.0546875
- tile_left: bfloat16 [12288, 1024], P('row', 'col'), may hold values from -0.4375 to 0.4375
- tile_right: bfloat16 [512, 12288], P('row', 'col'), may hold values from -0.625 to 0.625
- piece_owner: int32 [4, 1024], P('row', 'col'), may hold values from 0 to 32767
- omega_main: float32 [512, 512], replicated, may hold values from 0 to 1
- damping: float32 [512], replicated, may hold values from 0.05 to 1
- local_basis: bfloat16 [256, 256, 256], P(('row', 'col')), may hold values from -0.375 to 0.375
- local_omega: float32 [256, 256, 256], P(('row', 'col')), may hold values from 0 to 1
- local_left: bfloat16 [256, 256, 256], P(('row', 'col')), may hold values from -0.75 to 0.75
- local_right: bfloat16 [256, 256, 256], P(('row', 'col')), may hold values from -0.75 to 0.75
- local_owner: int32 [256, 256], P(('row', 'col')), may hold values from 0 to 32767
Outputs:
- solution: float32 [32768], P(('row', 'col'))
- residual: float32 [32768], P(('row', 'col'))
The draws below stay inside these ranges and needn't reach their ends.
All inputs are finite; a program needn't handle non-finite values.
Results may differ from the reference program's by a relative error of at most 0.00057.
Values may be sent and summed in bfloat16 or wider, within the bound.
No kernel may reach another device: no remote copies, remote signals or barrier semaphores. Data moves between devices by JAX's collectives and lax.ppermute only.
A program may use at most 128 MiB of HBM per device.

```python
import math
import jax
import jax.numpy as jnp
import numpy as np
from jax import lax

NORD = 12288
RANK = 512
SM = 256
SP = 256
PIECES = 128
ITERS = 2
TC = 1536
MCON = 32768
LOCAL = 256
N_ROW = 4
N_COL = 8


def with_ends(array, stream_key, low, high):
    shape = array.shape
    place = [jax.random.randint(jax.random.fold_in(stream_key, axis), (), 0, shape[axis]) for axis in range(len(shape))]
    array = array.at[tuple(place)].set(low)
    longest = shape.index(max(shape))
    place[longest] = (place[longest] + 1) % shape[longest]
    return array.at[tuple(place)].set(high)


def block_scale(key, dims, pieces, least, top_value):
    def one(position, shards_of):
        heights = jax.random.uniform(jax.random.fold_in(jax.random.fold_in(key, 6), position), (shards_of,), jnp.float32, least / len(pieces), top_value / len(pieces))
        return jnp.repeat(jnp.exp(heights), dims[position] // shards_of).reshape((-1,) + (1,) * (len(dims) - position - 1))

    loudness = one(*pieces[0])
    for cut in pieces[1:]:
        loudness = loudness * one(*cut)
    return loudness


def rank_table(number_of, skew):
    portions = [(1 << 20) // math.isqrt(rank ** skew) + 1 for rank in range(1, number_of + 1)]
    spread = 1 + sum(portions) // (1 << 30)
    return np.cumsum(np.array([max(1, weight // spread) for weight in portions]))


def ranked(stream_key, dims, amount, slope):
    listing = rank_table(amount, slope)
    pick = jax.random.randint(jax.random.fold_in(stream_key, 1), dims, 0, int(listing[amount - 1]))
    grade = jnp.searchsorted(jnp.asarray(listing, jnp.int32), pick, side="right")
    return jax.random.permutation(jax.random.fold_in(stream_key, 2), amount)[grade].astype(jnp.int32)


def normal_values(own_key, shape, width, limit, pieces=(), kind=jnp.bfloat16):
    loudness = block_scale(own_key, shape, pieces, -0.22, 0.18) if pieces else 1.0
    result = jax.random.normal(own_key, shape, jnp.float32) * width * loudness
    return jnp.minimum(jnp.maximum(result, -limit), limit).astype(kind)


def setup_inputs(seed: int = 0) -> dict:
    splits = jax.random.split(jax.random.key(seed), 13)
    right_side = normal_values(splits[0], (MCON,), 1.0, 6.0, ((0, 32),), jnp.float32)
    eigen_basis = normal_values(splits[1], (NORD, RANK), NORD ** -0.5, 0.0546875, ((0, 32),))
    tile_left = normal_values(splits[2], (NORD, N_COL * PIECES), (max(NORD // N_ROW // 16, 1)) ** -0.5, 0.4375, ((0, 4), (1, 8)))
    tile_right = normal_values(splits[3], (N_ROW * PIECES, N_COL * TC), (max(NORD // N_COL // 16, 1)) ** -0.5, 0.625, ((0, 4), (1, 8)))
    piece_owner = with_ends(ranked(splits[4], (N_ROW, N_COL * PIECES), MCON, 2), jax.random.fold_in(splits[4], 3), 0, MCON - 1).astype(jnp.int32)
    omega_main = jnp.clip(jax.random.uniform(splits[5], (RANK, RANK), jnp.float32, 0.0, 1.0), 0.0, 1.0)
    damping = jnp.clip(jax.random.uniform(splits[6], (RANK,), jnp.float32, 0.05, 1.0), 0.05, 1.0)
    local_basis = normal_values(splits[7], (LOCAL, SM, SM), SM ** -0.5, 0.375, ((0, 32),))
    local_omega = jnp.clip(1.0 * jax.random.uniform(splits[8], (LOCAL, SM, SM), jnp.float32) ** block_scale(splits[8], (LOCAL, SM, SM), ((0, 32),), -0.2, 0.2), 0.0, 1.0)
    local_left = normal_values(splits[9], (LOCAL, SP, SM), (SM // 4) ** -0.5, 0.75, ((0, 32),))
    local_right = normal_values(splits[10], (LOCAL, SP, SM), (SM // 4) ** -0.5, 0.75, ((0, 32),))
    local_owner = with_ends(ranked(splits[11], (LOCAL, SP), MCON, 1), jax.random.fold_in(splits[11], 3), 0, MCON - 1).astype(jnp.int32)
    return {"right_side": right_side, "eigen_basis": eigen_basis, "tile_left": tile_left, "tile_right": tile_right, "piece_owner": piece_owner, "omega_main": omega_main, "damping": damping, "local_basis": local_basis, "local_omega": local_omega, "local_left": local_left, "local_right": local_right, "local_owner": local_owner}


precise = lax.Precision.HIGHEST


def reference(right_side, eigen_basis, tile_left, tile_right, piece_owner, omega_main, damping, local_basis, local_omega, local_left, local_right, local_owner):
    row_len = NORD // N_ROW
    col_len = NORD // N_COL
    block_len = NORD // (N_ROW * N_COL)
    tile_count = N_ROW * N_COL
    blocked = eigen_basis.reshape(N_ROW, N_COL, block_len, RANK)
    owners = piece_owner.reshape(N_ROW, N_COL, PIECES).reshape(tile_count, PIECES)
    omega_sym = 0.5 * (omega_main + omega_main.T)
    local_sym = 0.5 * (local_omega + jnp.swapaxes(local_omega, 1, 2))
    counters = jnp.arange(tile_count, dtype=jnp.int32)
    contract = (((0,), (0,)), ((), ()))

    def fetch_tile(counter):
        tile_row = (counter // N_COL).astype(jnp.int32)
        tile_col = (counter % N_COL).astype(jnp.int32)
        left_part = lax.dynamic_slice(tile_left, (tile_row * row_len, tile_col * PIECES), (row_len, PIECES))
        right_part = lax.dynamic_slice(tile_right, (tile_row * PIECES, tile_col * col_len), (PIECES, col_len))
        return tile_row, tile_col, left_part, right_part

    def project(counter):
        tile_row, tile_col, left_part, right_part = fetch_tile(counter)
        basis_rows = lax.dynamic_slice_in_dim(eigen_basis, tile_row * row_len, row_len, 0)
        basis_cols = lax.dynamic_index_in_dim(blocked, tile_col, 1, keepdims=False).reshape(col_len, RANK)
        left_proj = lax.dot_general(left_part, basis_rows, contract, preferred_element_type=jnp.float32)
        right_proj = jnp.dot(right_part, basis_cols, preferred_element_type=jnp.float32)
        return left_proj.astype(jnp.bfloat16), right_proj.astype(jnp.bfloat16)

    left_projs, right_projs = lax.map(project, counters)
    local_lp = jnp.einsum("lps,lsk->lpk", local_left.astype(jnp.float32), local_basis.astype(jnp.float32)).astype(jnp.bfloat16)
    local_rp = jnp.einsum("lps,lsk->lpk", local_right.astype(jnp.float32), local_basis.astype(jnp.float32)).astype(jnp.bfloat16)
    left_float = local_lp.astype(jnp.float32)
    right_float = local_rp.astype(jnp.float32)

    def operate(dual_vec):
        def accumulate(field_sum, counter):
            tile_row, tile_col, left_part, right_part = fetch_tile(counter)
            coeffs = dual_vec[owners[counter]]
            scaled_right = (coeffs[:, None] * right_projs[counter].astype(jnp.float32)).astype(jnp.bfloat16)
            scaled_left = (coeffs[:, None] * left_projs[counter].astype(jnp.float32)).astype(jnp.bfloat16)
            row_terms = jnp.dot(left_part, scaled_right, preferred_element_type=jnp.float32)
            col_terms = lax.dot_general(right_part, scaled_left, contract, preferred_element_type=jnp.float32)
            field_sum = field_sum.at[tile_row].add(row_terms.reshape(N_COL, block_len, RANK))
            field_sum = field_sum.at[:, tile_col].add(col_terms.reshape(N_ROW, block_len, RANK))
            return field_sum, None

        field_sum, unused = lax.scan(accumulate, jnp.zeros((N_ROW, N_COL, block_len, RANK), jnp.float32), counters)
        field_half = field_sum.astype(jnp.bfloat16)
        curvature = lax.dot_general(eigen_basis, field_half.reshape(NORD, RANK), contract, preferred_element_type=jnp.float32)
        weights = omega_sym * curvature

        def evaluate(counter):
            tile_row, tile_col, left_part, right_part = fetch_tile(counter)
            field_rows = lax.dynamic_index_in_dim(field_half, tile_row, 0, keepdims=False).reshape(row_len, RANK)
            field_cols = lax.dynamic_index_in_dim(field_half, tile_col, 1, keepdims=False).reshape(col_len, RANK)
            left_field = lax.dot_general(left_part, field_rows, contract, preferred_element_type=jnp.float32)
            right_field = jnp.dot(right_part, field_cols, preferred_element_type=jnp.float32)
            left_proj = left_projs[counter].astype(jnp.float32)
            right_proj = right_projs[counter].astype(jnp.float32)
            left_rest = left_field - jnp.dot(left_proj, curvature, precision=precise)
            right_rest = right_field - jnp.dot(right_proj, curvature, precision=precise)
            weighted = jnp.dot(right_proj, weights, precision=precise)
            inner_sum = left_proj * weighted + left_rest * (damping * right_proj) + (damping * left_proj) * right_rest
            return 2.0 * jnp.sum(inner_sum, axis=1)

        big_values = lax.map(evaluate, counters)
        local_coeffs = dual_vec[local_owner]
        scaled = local_coeffs[:, :, None] * left_float
        half_t = jnp.einsum("lpa,lpb->lab", scaled, right_float, precision=precise)
        gram_mat = half_t + jnp.swapaxes(half_t, 1, 2)
        local_w = local_sym * gram_mat
        mixed_rows = jnp.einsum("lpb,lba->lpa", right_float, local_w, precision=precise)
        local_values = 2.0 * jnp.sum(left_float * mixed_rows, axis=2)
        totals = jnp.zeros((MCON,), jnp.float32).at[owners.reshape(-1)].add(big_values.reshape(-1))
        totals = totals.at[local_owner.reshape(-1)].add(local_values.reshape(-1))
        return dual_vec + totals

    solution = jnp.zeros_like(right_side)
    residual = right_side
    direction = right_side
    norm_now = jnp.sum(residual * residual)
    for counter in range(ITERS):
        applied = operate(direction)
        step_size = norm_now / jnp.sum(direction * applied)
        solution = solution + step_size * direction
        residual = residual - step_size * applied
        norm_next = jnp.sum(residual * residual)
        direction = residual + (norm_next / norm_now) * direction
        norm_now = norm_next
    return solution, residual
```

```python
import jax
import jax.numpy as jnp
from jax import lax
from jax.sharding import PartitionSpec as P

LANES = 128
BOTH = ("row", "col")
f32 = jnp.float32
bf16 = jnp.bfloat16


def tdot(a, b):
    return lax.dot_general(a, b, (((0,), (0,)), ((), ())), preferred_element_type=f32)


def mdot(a, b):
    return jnp.dot(a, b, preferred_element_type=f32)


def halves(x):
    top = lax.reduce_precision(x, 8, 7)
    return top.astype(bf16), (x - top).astype(bf16)


def onehot(index, size):
    return index[:, None] == lax.broadcasted_iota(jnp.int32, (index.shape[0], size), 1)


def spread(x, devices):
    return lax.all_to_all(jnp.broadcast_to(x[None], (devices,) + x.shape), BOTH, 0, 0, tiled=True)


def local(
    n_row,
    n_col,
    right_side,
    eigen_basis,
    tile_left,
    tile_right,
    piece_owner,
    omega_main,
    damping,
    local_basis,
    local_omega,
    local_left,
    local_right,
    local_owner,
):
    devices = n_row * n_col
    pieces = tile_left.shape[1]
    height, rank = eigen_basis.shape
    chunk = right_side.shape[0] // LANES
    heads = chunk * devices
    row_at = lax.axis_index("row")
    col_at = lax.axis_index("col")
    at = row_at * n_col + col_at

    basis_rows = lax.all_gather(eigen_basis, "col", axis=0, tiled=True)
    basis_cols = lax.all_gather(eigen_basis, "row", axis=0, tiled=True)
    own_words = jnp.concatenate(
        [right_side.reshape(chunk, LANES), piece_owner.reshape(-1, LANES).astype(f32)], axis=0
    )
    words = spread(own_words, devices)
    u_block = lax.all_to_all(tile_left.reshape(n_col, height, pieces), "col", 0, 0, tiled=True)
    u_block = jnp.swapaxes(u_block, 0, 1).reshape(height, n_col * pieces)
    v_block = jnp.swapaxes(tile_right.reshape(pieces, n_row, height), 0, 1)
    v_block = lax.all_to_all(v_block, "row", 0, 0, tiled=True).reshape(n_row * pieces, height)
    left_proj = tdot(tile_left, basis_rows).astype(bf16)
    right_proj = mdot(tile_right, basis_cols).astype(bf16)
    projs = lax.all_gather(
        jnp.concatenate([left_proj, right_proj], axis=1), BOTH, axis=0, tiled=True
    )
    left_all = projs[:, :rank]
    right_all = projs[:, rank:]
    right_group = lax.dynamic_slice_in_dim(right_all, row_at * n_col * pieces, n_col * pieces, 0)
    left_group = lax.dynamic_index_in_dim(
        left_all.reshape(n_row, n_col, pieces, rank), col_at, 1, keepdims=False
    ).reshape(n_row * pieces, rank)

    right_full = words[:, :chunk].reshape(heads, LANES)
    owners_all = words[:, chunk:].astype(jnp.int32).reshape(n_row, n_col, pieces)
    owners_u = lax.dynamic_index_in_dim(owners_all, row_at, 0, keepdims=False).reshape(-1)
    owners_v = lax.dynamic_index_in_dim(owners_all, col_at, 1, keepdims=False).reshape(-1)
    local_flat = local_owner.reshape(-1)
    owners_read = jnp.concatenate([owners_all.reshape(-1), local_flat])
    owners_write = jnp.concatenate([owners_u, owners_v, local_flat])
    read_head = onehot(owners_read // LANES, heads).astype(bf16)
    read_lane = onehot(owners_read % LANES, LANES)
    write_head = onehot(owners_write // LANES, heads).astype(bf16)
    write_lane = onehot(owners_write % LANES, LANES)

    omega_sym = 0.5 * (omega_main + omega_main.T)
    bend = damping[None, :] - 0.5 * omega_sym
    local_sym = 0.5 * (local_omega + jnp.swapaxes(local_omega, 1, 2))
    local_lp = jnp.einsum(
        "lps,lsk->lpk", local_left, local_basis, preferred_element_type=f32
    ).astype(bf16)
    local_rp = jnp.einsum(
        "lps,lsk->lpk", local_right, local_basis, preferred_element_type=f32
    ).astype(bf16)
    left_float = local_lp.astype(f32)

    def partial(vector):
        top, low = halves(vector)
        rows = mdot(read_head, jnp.concatenate([top, low], axis=1))
        rows = rows[:, :LANES] + rows[:, LANES:]
        coeffs = jnp.sum(jnp.where(read_lane, rows, 0.0), axis=1)
        coeffs_all = coeffs[: devices * pieces]
        grid = coeffs_all.reshape(n_row, n_col, pieces)
        coeffs_u = lax.dynamic_index_in_dim(grid, row_at, 0, keepdims=False).reshape(-1)
        coeffs_v = lax.dynamic_index_in_dim(grid, col_at, 1, keepdims=False).reshape(-1)
        local_coeffs = coeffs[devices * pieces :].reshape(local_owner.shape)

        half_k = tdot(left_all, (coeffs_all[:, None] * right_all.astype(f32)).astype(bf16))
        curvature = half_k + half_k.T
        scaled_right = (coeffs_u[:, None] * right_group.astype(f32)).astype(bf16)
        scaled_left = (coeffs_v[:, None] * left_group.astype(f32)).astype(bf16)
        field = mdot(u_block, scaled_right) + tdot(v_block, scaled_left)
        field = field.astype(bf16).astype(f32)
        bent_top, bent_low = halves(curvature * bend)
        pull = field * damping - (mdot(eigen_basis, bent_top) + mdot(eigen_basis, bent_low))
        pull_top, pull_low = halves(pull)
        back_u = tdot(u_block, pull_top) + tdot(u_block, pull_low)
        back_v = mdot(v_block, pull_top) + mdot(v_block, pull_low)
        values_u = 2.0 * jnp.sum(back_u * right_group.astype(f32), axis=1)
        values_v = 2.0 * jnp.sum(back_v * left_group.astype(f32), axis=1)

        scaled = (local_coeffs[:, :, None] * left_float).astype(bf16)
        half_t = jnp.einsum("lpa,lpb->lab", scaled, local_rp, preferred_element_type=f32)
        local_w = (local_sym * (half_t + jnp.swapaxes(half_t, 1, 2))).astype(bf16)
        mixed = jnp.einsum("lpb,lba->lpa", local_rp, local_w, preferred_element_type=f32)
        local_values = 2.0 * jnp.sum(left_float * mixed, axis=2)

        values = jnp.concatenate([values_u, values_v, local_values.reshape(-1)])
        top, low = halves(values)
        top = jnp.where(write_lane, top[:, None], jnp.zeros((), bf16))
        low = jnp.where(write_lane, low[:, None], jnp.zeros((), bf16))
        totals = tdot(write_head, jnp.concatenate([top, low], axis=1))
        return totals[:, :LANES] + totals[:, LANES:]

    def own(vector):
        return lax.dynamic_slice_in_dim(vector, at * chunk, chunk, 0)

    norm_now = jnp.sum(right_full * right_full)
    parts = partial(right_full).reshape(devices, chunk, LANES)
    share = jnp.sum(lax.all_to_all(parts, BOTH, 0, 0, tiled=True), axis=0)
    applied = right_full + spread(share, devices).reshape(heads, LANES)
    step_one = norm_now / jnp.sum(right_full * applied)
    residual = right_full - step_one * applied
    norm_next = jnp.sum(residual * residual)
    direction = residual + norm_next / norm_now * right_full
    totals = partial(direction)
    term = jnp.broadcast_to(jnp.sum(direction * totals), (devices, 1, LANES))
    parts = jnp.concatenate([totals.reshape(devices, chunk, LANES), term], axis=1)
    parts = jnp.sum(lax.all_to_all(parts, BOTH, 0, 0, tiled=True), axis=0)
    inner = jnp.sum(direction * direction) + parts[chunk, 0]
    step_two = norm_next / inner
    own_direction = own(direction)
    solution = step_one * right_side.reshape(chunk, LANES) + step_two * own_direction
    left_over = own(residual) - step_two * (own_direction + parts[:chunk])
    return solution.reshape(-1), left_over.reshape(-1)


def solution(mesh):
    n_row = mesh.shape["row"]
    n_col = mesh.shape["col"]
    placed = (
        P(BOTH),
        P(BOTH, None),
        P("row", "col"),
        P("row", "col"),
        P("row", "col"),
        P(),
        P(),
        P(BOTH, None, None),
        P(BOTH, None, None),
        P(BOTH, None, None),
        P(BOTH, None, None),
        P(BOTH, None),
    )
    return jax.shard_map(
        lambda *arrays: local(n_row, n_col, *arrays),
        mesh=mesh,
        in_specs=placed,
        out_specs=(P(BOTH), P(BOTH)),
        check_vma=False,
    )
```

```python
import functools

import jax
import jax.numpy as jnp
from jax import lax
from jax.experimental import pallas as pl
from jax.experimental.pallas import tpu as pltpu
from jax.sharding import PartitionSpec as P


LANES = 128
SUB = 8
BOTH = ("row", "col")
f32 = jnp.float32
bf16 = jnp.bfloat16
VMEM_LIMIT = 56 * 1024 * 1024


def tdot(a, b):
    return lax.dot_general(a, b, (((0,), (0,)), ((), ())), preferred_element_type=f32)


def mdot(a, b):
    return jnp.dot(a, b, preferred_element_type=f32)


def exchange(x, axes):
    return lax.all_to_all(x, axes, 0, 0, tiled=True)


def spread(x, axes, size):
    return exchange(jnp.broadcast_to(x[None], (size,) + x.shape), axes)


def swap(x, axis, size, mask):
    return lax.ppermute(x, axis, [(i, i ^ mask) for i in range(size)])


def shift(x, axis, size, step):
    return lax.ppermute(x, axis, [(i, (i + step) % size) for i in range(size)])


def total(x):
    return jnp.sum(jnp.sum(x, axis=1, keepdims=True), axis=0, keepdims=True)


def halves(x):
    top = x.astype(bf16)
    return jnp.concatenate([top, (x - top.astype(f32)).astype(bf16)], axis=1)


def pick(vector, heads, lanes):
    rows = mdot(heads, halves(vector))
    rows = rows[:, :LANES] + rows[:, LANES:]
    return jnp.sum(rows * lanes.astype(f32), axis=1, keepdims=True)


def drop(values, heads_t, lanes):
    sums = mdot(heads_t, halves(values * lanes.astype(f32)))
    return sums[:, :LANES] + sums[:, LANES:]


def wide(spots, ref):
    return jnp.concatenate([ref[spots[j]] for j in range(ref.shape[0])], axis=1)


def stacked(refs):
    return jnp.concatenate([ref[...] for ref in refs], axis=0)


def curve(vector, heads, lanes, left_row, left_pair, right_row, right_pair, k_out):
    coeffs = pick(vector, heads[...], lanes[...])
    rank = left_row.shape[2]
    half = rank // 2
    grams = jnp.zeros((rank, rank), f32)
    count = heads.shape[0] // 2
    for n, (left, right) in enumerate(((left_row, right_row), (left_pair, right_pair))):
        part = coeffs[n * count : (n + 1) * count]
        scaled = (part * right[...].reshape(count, rank).astype(f32)).astype(bf16)
        grams = grams + tdot(left[...].reshape(count, rank), scaled)
    cross = grams[:half, half:] + grams[half:, :half].T
    first, last = grams[:half, :half], grams[half:, half:]
    blocks = jnp.concatenate([first + first.T, cross, last + last.T], axis=1).astype(bf16)
    for n in range(blocks.shape[1] // LANES):
        k_out[n * half : (n + 1) * half, :] = blocks[:, n * LANES : (n + 1) * LANES]


def curve_first(vector, *refs):
    curve(vector[...], *refs)


def curve_second(right, totals, *refs):
    *rest, k_out, direction_out, residual_out, steps_out = refs
    first = right[...]
    applied = first + totals[...]
    norm_now = total(first * first)
    step = norm_now / total(first * applied)
    residual = first - step * applied
    norm_next = total(residual * residual)
    direction = residual + norm_next / norm_now * first
    direction_out[...] = direction
    residual_out[...] = residual
    steps_out[0:1, :] = jnp.broadcast_to(step, (1, LANES))
    steps_out[1:2, :] = jnp.broadcast_to(norm_next, (1, LANES))
    steps_out[2:3, :] = jnp.broadcast_to(total(direction * direction), (1, LANES))
    steps_out[3:, :] = jnp.zeros((SUB - 3, LANES), f32)
    curve(direction, *rest, k_out)


def front(spots, vector, heads, lanes, group_right, u_block, v_block, *refs):
    *group_left, s_out = refs
    coeffs = pick(vector[...], heads[...], lanes[...])
    count, rank = heads.shape[0], group_right.shape[2]
    count = count - len(group_left) * group_left[0].shape[0]
    right = group_right[...].reshape(count, rank).astype(f32)
    left = stacked(group_left).astype(f32)
    field = mdot(wide(spots, u_block), (coeffs[:count] * right).astype(bf16))
    field = field + mdot(v_block[...], (coeffs[count:] * left).astype(bf16))
    s_out[...] = field.astype(bf16)


def right_project(own_right, *refs):
    *sides, out, v_out = refs
    rank = out.shape[1]
    out[...] = tdot(
        own_right[...].reshape(-1, own_right.shape[2]),
        jnp.concatenate([ref[:, :rank] for ref in sides], axis=0),
    ).astype(bf16)
    v_out[...] = jnp.concatenate([ref[:, rank:] for ref in sides], axis=1)


def left_project(order, basis, u_block, far, near):
    count = far.shape[0]
    for out, base in ((far, 0), (near, count)):
        factors = jnp.concatenate([u_block[order[base + n]] for n in range(count)], axis=1)
        out[...] = tdot(factors, basis[...]).astype(out.dtype).reshape(out.shape)


def block_values(n, vector, heads, lanes, left, right, weights):
    count = left.shape[0]
    rows = slice(n * count, (n + 1) * count)
    coeffs = pick(vector[...], heads[rows, :], lanes[rows, :])
    scaled = (coeffs * left.astype(f32)).astype(bf16)
    half_t = tdot(scaled, right)
    bent = (weights * (half_t + half_t.T)).astype(bf16)
    mixed = mdot(right, bent)
    return 2.0 * jnp.sum(left.astype(f32) * mixed, axis=1, keepdims=True)


def gather_sums(values, heads_t, lanes, out):
    sums = drop(jnp.concatenate(values, axis=0), heads_t[...], lanes[...])
    at = pl.program_id(0)

    @pl.when(at == 0)
    def _():
        out[...] = sums

    @pl.when(at > 0)
    def _():
        out[...] += sums


def blocks_ready(basis, left, right, omega, left_out, right_out, weights_out):
    for n in range(left.shape[0]):
        left_out[n] = mdot(left[n], basis[n]).astype(bf16)
        right_out[n] = mdot(right[n], basis[n]).astype(bf16)
        weights_out[n] = 0.5 * (omega[n] + omega[n].T)


def blocks_step(vector, heads, lanes, heads_t, left, right, weights, out):
    values = [
        block_values(n, vector, heads, lanes, left[n], right[n], weights[n])
        for n in range(left.shape[0])
    ]
    gather_sums(values, heads_t, lanes, out)


def back(spots, field, k_own, k_other, bend, damping, basis, heads_t, lanes, local_sums,
         group_right, u_block, v_block, *group_left):
    rank = basis.shape[1]
    half = rank // 2
    width = rank // LANES
    curvature = k_own[...].astype(f32) + k_other[...].astype(f32)
    parts = [curvature[n * half : (n + 1) * half, :] for n in range(width + width // 2)]
    top = jnp.concatenate(parts[:width], axis=1)
    low = jnp.concatenate([top[:, half:].T] + parts[width:], axis=1)
    curvature = jnp.concatenate([top, low], axis=0)
    bent = (curvature * bend[...]).astype(bf16)
    pull = field[...].astype(f32) * damping[...] - mdot(basis[...], bent)
    pull = pull.astype(bf16)
    right = group_right[...].reshape(-1, rank).astype(f32)
    back_u = tdot(wide(spots, u_block), pull) * right
    back_v = tdot(v_block[...], pull) * stacked(group_left).astype(f32)
    values_u = jnp.sum(back_u, axis=1, keepdims=True)
    values_v = jnp.sum(back_v, axis=1, keepdims=True)
    values = 2.0 * jnp.concatenate([values_u, values_v], axis=0)
    return local_sums[...] + drop(values, heads_t[...], lanes[...])


def back_first(*refs):
    *rest, out = refs
    out[...] = back(*rest)


def back_second(spots, direction, *refs):
    *rest, out = refs
    sums = back(spots, *rest)
    devices, rows, _ = out.shape
    out[:, : rows - SUB, :] = sums.reshape(devices, rows - SUB, LANES)
    term = total(direction[...] * sums)
    out[:, rows - SUB :, :] = jnp.broadcast_to(term.reshape(1, 1, 1), (devices, SUB, LANES))


def finish(at, parts, direction, residual, right_own, steps, answer, left_over):
    chunk = right_own.shape[0]
    sums = jnp.sum(parts[...], axis=0)
    step_two = steps[1:2, :] / (steps[2:3, :] + sums[chunk : chunk + 1, :])
    rows = pl.ds(at[0] * chunk, chunk)
    way = direction[rows, :]
    answer[...] = steps[0:1, :] * right_own[...] + step_two * way
    left_over[...] = residual[rows, :] - step_two * (way + sums[:chunk])


def kernel(body, outs, count, order=False):
    specs = [pl.BlockSpec(memory_space=pltpu.VMEM)] * count
    if order:
        specs = [pl.BlockSpec(memory_space=pltpu.SMEM)] + specs
    return pl.pallas_call(
        body,
        in_specs=specs,
        out_shape=outs,
        compiler_params=pltpu.CompilerParams(vmem_limit_bytes=VMEM_LIMIT),
    )


def blocks_kernel(heads, pieces, side, count, ready):
    batch = 2 if count % 2 == 0 else 1
    whole = pl.BlockSpec((heads, LANES), lambda l: (0, 0))
    square = pl.BlockSpec((batch, side, side), lambda l: (l, 0, 0))
    factor = pl.BlockSpec((batch, pieces, side), lambda l: (l, 0, 0))
    if ready:
        body = blocks_ready
        specs = [square, factor, factor, square]
        outs = (
            jax.ShapeDtypeStruct((count, pieces, side), bf16),
            jax.ShapeDtypeStruct((count, pieces, side), bf16),
            jax.ShapeDtypeStruct((count, side, side), f32),
        )
        out_specs = (factor, factor, square)
    else:
        body = blocks_step
        specs = [
            whole,
            pl.BlockSpec((batch * pieces, heads), lambda l: (l, 0)),
            pl.BlockSpec((batch * pieces, LANES), lambda l: (l, 0)),
            pl.BlockSpec((heads, batch * pieces), lambda l: (0, l)),
            factor,
            factor,
            square,
        ]
        outs, out_specs = jax.ShapeDtypeStruct((heads, LANES), f32), whole
    return pl.pallas_call(
        body,
        grid=(count // batch,),
        in_specs=specs,
        out_specs=out_specs,
        out_shape=outs,
        compiler_params=pltpu.CompilerParams(vmem_limit_bytes=VMEM_LIMIT),
    )


def local(
    n_row,
    n_col,
    right_side,
    eigen_basis,
    tile_left,
    tile_right,
    piece_owner,
    omega_main,
    damping,
    local_basis,
    local_omega,
    local_left,
    local_right,
    local_owner,
):
    devices = n_row * n_col
    pieces = tile_left.shape[1]
    height, rank = eigen_basis.shape
    chunk = right_side.shape[0] // LANES
    heads = chunk * devices
    side = local_basis.shape[1]
    blocks, local_pieces = local_owner.shape
    row_at = lax.axis_index("row")
    col_at = lax.axis_index("col")
    at = row_at * n_col + col_at
    shape = jax.ShapeDtypeStruct

    def run(body, outs, *arrays):
        return kernel(body, outs, len(arrays))(*arrays)

    def run_ordered(body, outs, *arrays):
        return kernel(body, outs, len(arrays), True)(spots, *arrays)

    own_words = jnp.concatenate(
        [right_side.reshape(chunk, LANES), piece_owner.reshape(-1, LANES).astype(f32)], axis=0
    )
    turned = jnp.transpose(tile_right.reshape(pieces, n_row, height), (1, 2, 0))
    own_right = [
        lax.dynamic_index_in_dim(turned, row_at ^ m, 0, keepdims=False) for m in range(n_row)
    ]
    sides = [jnp.concatenate([eigen_basis, part], axis=1) for part in own_right]
    sides = sides[:1] + [swap(sides[m], "row", n_row, m) for m in range(1, n_row)]
    u_block = exchange(tile_left.reshape(n_col, height, pieces), "col")

    locals_ready = blocks_kernel(heads, local_pieces, side, blocks, True)(
        local_basis, local_left, local_right, local_omega
    )
    own_words, u_block, locals_ready = lax.optimization_barrier((own_words, u_block, locals_ready))
    words = spread(own_words, BOTH, devices)
    lines = n_col // 2
    line_at, odd = col_at // 2, col_at % 2
    half_shape = (lines, pieces, rank)
    aims = 2 * jnp.arange(lines, dtype=jnp.int32)
    far, near = kernel(
        left_project, (shape(half_shape, bf16), shape(half_shape, f32)), 2, True
    )(jnp.concatenate([aims + 1 - odd, aims + odd]), eigen_basis, u_block)
    sides[1], far = lax.optimization_barrier((sides[1], far))
    right_proj, v_block = run(
        right_project,
        (shape((pieces, rank), bf16), shape((height, n_row * pieces), bf16)),
        jnp.stack(own_right), *sides,
    )
    far = swap(far, "col", n_col, 1)
    line = [right_proj] + [shift(right_proj, "col", n_col, 2 * k) for k in range(1, lines)]
    far, line = lax.optimization_barrier((far, line))
    line = jnp.stack(line)
    across = swap(line, "col", n_col, 1)

    def near_sum(k):
        at_line = (line_at + k) % lines
        here = lax.dynamic_index_in_dim(near, at_line, 0, keepdims=False)
        return here + lax.dynamic_index_in_dim(far, at_line, 0, keepdims=False).astype(f32)

    terms = [shift(near_sum(k).astype(bf16), "col", n_col, 2 * k) for k in range(1, lines)]
    terms, across = lax.optimization_barrier((terms, across))
    left_proj = near_sum(0)
    for term in terms:
        left_proj = left_proj + term.astype(f32)
    left_proj = left_proj.astype(bf16)
    right_row = jnp.concatenate([line, across], axis=0)
    group_left = [left_proj] + [swap(left_proj, "row", n_row, m) for m in range(1, n_row)]
    left_line = [left_proj] + [
        shift(left_proj, "col", n_col, 2 * k) for k in range(1, lines)
    ]
    left_row = jnp.stack(left_line + [swap(part, "col", n_col, 1) for part in left_line])
    left_pair, right_pair = swap(left_row, "row", n_row, 1), swap(right_row, "row", n_row, 1)
    steps = jnp.arange(n_col, dtype=jnp.int32)
    spots = 2 * ((line_at - steps % lines) % lines) + (odd + steps // lines) % 2
    spots = spots.astype(jnp.int32)

    right_full = words[:, :chunk].reshape(heads, LANES)
    owners_all = words[:, chunk:].astype(jnp.int32).reshape(n_row, n_col, pieces)
    owners_row = jnp.take(owners_all[row_at], spots, axis=0).reshape(-1)
    owners_pair = jnp.take(owners_all[row_at ^ 1], spots, axis=0).reshape(-1)
    owners = jnp.concatenate([owners_row] + [owners_all[row_at ^ m, col_at] for m in range(n_row)])
    owners_k = jnp.concatenate([owners_row, owners_pair])

    def table(index, size):
        return (index[:, None] == jnp.arange(size, dtype=jnp.int32)[None, :]).astype(bf16)

    def table_t(index, size):
        return (jnp.arange(size, dtype=jnp.int32)[:, None] == index[None, :]).astype(bf16)

    local_flat = local_owner.reshape(-1)
    k_heads, k_lanes = table(owners_k // LANES, heads), table(owners_k % LANES, LANES)
    tile_heads, tile_lanes = table(owners // LANES, heads), table(owners % LANES, LANES)
    tile_heads_t = table_t(owners // LANES, heads)
    block_heads, block_lanes = table(local_flat // LANES, heads), table(local_flat % LANES, LANES)
    block_heads_t = table_t(local_flat // LANES, heads)

    weight = damping.reshape(1, rank)
    bend = weight - 0.25 * (omega_main + omega_main.T)

    def blocked(vector):
        return blocks_kernel(heads, local_pieces, side, blocks, False)(
            vector, block_heads, block_lanes, block_heads_t, *locals_ready
        )

    k_rows = 3 * (rank // 2) * (rank // 2) // LANES
    k_shape = shape((k_rows, LANES), bf16)
    full_shape = shape((heads, LANES), f32)
    curve_rest = (k_heads, k_lanes, left_row, left_pair, right_row, right_pair)
    tile_rest = (right_row, u_block, v_block, *group_left)

    def fronted(vector):
        return run_ordered(
            front, shape((height, rank), bf16), vector, tile_heads, tile_lanes, *tile_rest
        )

    def back_args(field, k_part, sums):
        k_other = swap(k_part, "row", n_row, 2)
        return (field, k_part, k_other, bend, weight, eigen_basis, tile_heads_t, tile_lanes, sums, *tile_rest)

    sums = blocked(right_full)
    k_part = run(curve_first, k_shape, right_full, *curve_rest)
    parts = run_ordered(back_first, full_shape, *back_args(fronted(right_full), k_part, sums))
    share = jnp.sum(exchange(parts.reshape(devices, chunk, LANES), BOTH), axis=0)
    totals = spread(share, BOTH, devices).reshape(heads, LANES)
    k_part, direction, residual, steps = run(
        curve_second,
        (k_shape, full_shape, full_shape, shape((SUB, LANES), f32)),
        right_full, totals, *curve_rest,
    )
    sums = blocked(direction)
    parts = run_ordered(
        back_second,
        shape((devices, chunk + SUB, LANES), f32),
        direction, *back_args(fronted(direction), k_part, sums),
    )
    own_shape = shape((chunk, LANES), f32)
    answer, left_over = kernel(finish, (own_shape, own_shape), 5, True)(
        jnp.full((1,), at, jnp.int32),
        exchange(parts, BOTH), direction, residual, right_side.reshape(chunk, LANES), steps,
    )
    return answer.reshape(-1), left_over.reshape(-1)


def solution(mesh):
    placed = (
        P(BOTH),
        P(BOTH, None),
        P("row", "col"),
        P("row", "col"),
        P("row", "col"),
        P(),
        P(),
        P(BOTH, None, None),
        P(BOTH, None, None),
        P(BOTH, None, None),
        P(BOTH, None, None),
        P(BOTH, None),
    )
    return jax.shard_map(
        functools.partial(local, mesh.shape["row"], mesh.shape["col"]),
        mesh=mesh,
        in_specs=placed,
        out_specs=(P(BOTH), P(BOTH)),
        check_vma=False,
    )
```
